32 devices in a mesh: dp: 8 (over z, x), patch: 4 (over y, core).
Axes of the slice: x: 2, y: 2, z: 4, core: 2. Of those that a mesh axis runs over, the one named last changes fastest.
Arguments:
- query_rows: bfloat16 [8, 512, 576], P('dp', 'patch'), may hold values from -6 to 6
- key_rows: bfloat16 [8, 512, 576], P('dp', 'patch'), may hold values from -6 to 6
- value_rows: bfloat16 [8, 512, 576], P('dp', 'patch'), may hold values from -6 to 6
- out_weight: bfloat16 [576, 1152], replicated, may hold values from -0.25 to 0.25
- target: bfloat16 [8, 512, 1152], P('dp', 'patch'), may hold values from -6 to 6
- lengths: int32 [8], P('dp'), may hold values from 64 to 512
- segments: int32 [8, 512], P('dp', 'patch'), may hold values from 0 to 7, never falling along the last dimension, each value on 1 to 256 neighbouring positions
Outputs:
- query_grad: float32 [8, 512, 576], P('dp', 'patch')
- key_grad: float32 [8, 512, 576], P('dp', 'patch')
- value_grad: float32 [8, 512, 576], P('dp', 'patch')
- weight_grad: float32 [576, 1152], P('patch', 'dp')
- loss: float32 [], replicated
The draws below stay inside these ranges and needn't reach their ends.
All inputs are finite; a program needn't handle non-finite values.
Results may differ from the reference program's by a relative error of at most 0.024.
Values may be sent and summed in bfloat16 or wider, within the bound.
A program may use at most 64 MiB of HBM per device.

```python
import math
import jax
import jax.numpy as jnp
import numpy as np
from jax import lax

WIDTH = 1152
HEADS = 8
HEAD_DIM = 72
TOK_DEV = 128
FEAT = 576
SEQ = 512
SAMPLES = 8


def draw_rows(key, salt, chosen_rows):
    fresh_key = jax.random.fold_in(key, salt)
    sampled = jnp.clip(1.5 * jax.random.normal(fresh_key, (SAMPLES, SEQ, FEAT), jnp.float32), -6.0, 6.0)
    return sampled.astype(jnp.bfloat16)


def draw_query_rows(key, part):
    positions = jnp.arange(SEQ)
    return draw_rows(key, 1, positions % TOK_DEV == 0)


def draw_key_rows(key, part):
    positions = jnp.arange(SEQ)
    return draw_rows(key, 2, positions % TOK_DEV == 0)


def plant(entries, key, low, largest):
    longest = entries.shape.index(max(entries.shape))
    spots = []
    for shift in (0, 1):
        where = [jax.random.randint(jax.random.fold_in(key, axis), (), 0, length) for axis, length in enumerate(entries.shape)]
        where[longest] = (where[longest] + shift) % entries.shape[longest]
        spots.append(tuple(where))
    return entries.at[spots[0]].set(low).at[spots[1]].set(largest)


def steps_of(stream_key, extent, split, least, largest):
    level = 1.0
    for position, shards_of in split:
        heights = jax.random.uniform(jax.random.fold_in(jax.random.fold_in(stream_key, 6), position), (shards_of,), jnp.float32, least / len(split), largest / len(split))
        level = level * jnp.repeat(jnp.exp(heights), extent[position] // shards_of).reshape((-1,) + (1,) * (len(extent) - 1 - position))
    return level


def profile(count, total, most, skew):
    weights = [(1 << 20) // math.isqrt(rank ** skew) + 1 for rank in range(2, count + 1)]
    surplus, counts = total - most - (count - 1), [1] * (count - 1)
    while surplus > 0:
        candidates = [i for i in range(count - 1) if counts[i] < most]
        pool, remaining = sum([weights[i] for i in candidates]), surplus
        for i in candidates:
            more = min(most - counts[i], max(1, remaining * weights[i] // pool), surplus)
            counts[i] = counts[i] + more
            surplus = surplus - more
    return np.array([most] + counts)


def uneven_parts(key, number_of, total, most, skew):
    if number_of == 2:
        one = jax.random.randint(key, (), max(1, total - most), min(most, total - 1) + 1)
        return jnp.stack([one, total - one])
    tallies = jnp.asarray(profile(number_of, total, most, skew), jnp.int32)
    pairs = (number_of - 1) // 2
    donor, sink = tallies[1:1 + 2 * pairs:2], tallies[2:2 + 2 * pairs:2]
    slack = jnp.minimum(donor - 1, most - sink)
    shifted = jax.random.randint(jax.random.fold_in(key, 1), (pairs,), 0, 1 << 20) % (slack + 1)
    tallies = tallies.at[1:1 + 2 * pairs:2].set(donor - shifted).at[2:2 + 2 * pairs:2].set(sink + shifted)
    return tallies[jax.random.permutation(jax.random.fold_in(key, 2), number_of)]


def normal_values(rng, shape, spread, most, split=(), kind=jnp.bfloat16):
    array = spread * jax.random.normal(rng, shape, jnp.float32)
    if split:
        array = array * steps_of(rng, shape, split, -0.22, 0.18)
    return jnp.clip(array, -most, most).astype(kind)


def setup_inputs(seed: int = 0) -> dict:
    arg_keys = jax.random.split(jax.random.key(seed), 8)
    query_rows = draw_query_rows(jax.random.fold_in(arg_keys[7], 71), 0)
    key_rows = draw_key_rows(jax.random.fold_in(arg_keys[7], 71), 0)
    value_rows = normal_values(arg_keys[2], (SAMPLES, SEQ, FEAT), 1.0, 6.0, ((0, 8), (1, 4)))
    out_weight = normal_values(arg_keys[3], (FEAT, WIDTH), FEAT ** -0.5, 0.25)
    target = normal_values(arg_keys[4], (SAMPLES, SEQ, WIDTH), 1.0, 6.0, ((0, 8), (1, 4)))
    lengths = plant(jax.random.randint(arg_keys[5], (SAMPLES,), SEQ // 8, SEQ + 1), jax.random.fold_in(arg_keys[5], 1), SEQ // 8, SEQ).astype(jnp.int32)
    segments = jax.vmap(lambda own: jnp.searchsorted(jnp.cumsum(uneven_parts(own, 8, SEQ, SEQ // 2, 2)), jnp.arange(SEQ), side="right"))(jax.random.split(arg_keys[6], SAMPLES)).reshape((SAMPLES, SEQ)).astype(jnp.int32)
    return {"query_rows": query_rows, "key_rows": key_rows, "value_rows": value_rows, "out_weight": out_weight, "target": target, "lengths": lengths, "segments": segments}


NEG_LARGE = -1e+30

def widen(value):
    return lax.optimization_barrier(value).astype(jnp.float32)

def one_sample(packed, out_weight):
    query_rows, key_rows, value_rows, target_rows, length, segment_row = packed
    score_scale = 1.0 / math.sqrt(HEAD_DIM)
    query_heads = query_rows.astype(jnp.float32).reshape(SEQ, HEADS, HEAD_DIM)
    key_heads = key_rows.astype(jnp.float32).reshape(SEQ, HEADS, HEAD_DIM)
    value_heads = value_rows.astype(jnp.float32).reshape(SEQ, HEADS, HEAD_DIM)
    live = lax.iota(jnp.int32, SEQ) < length
    group = jnp.where(live, segment_row, -1)
    allowed = (group[:, None] == group[None, :])[None, :, :]
    scores = jnp.einsum('qhe,khe->hqk', query_heads, key_heads) * score_scale
    masked = jnp.where(allowed, scores, NEG_LARGE)
    row_max = lax.optimization_barrier(jnp.max(masked, axis=2))
    probs = jnp.where(allowed, jnp.exp(masked - row_max[:, :, None]), 0.0)
    denom = lax.optimization_barrier(jnp.sum(probs, axis=2))
    weights = widen(probs.astype(jnp.bfloat16))
    accum = jnp.einsum('hqk,khe->qhe', weights, value_heads)
    attn = (accum / denom.T[:, :, None]).reshape(SEQ, FEAT).astype(jnp.bfloat16)
    log_norm = row_max + jnp.log(denom)
    output = jnp.dot(attn, out_weight, preferred_element_type=jnp.float32)
    error = jnp.where(live[:, None], output - target_rows.astype(jnp.float32), 0.0)
    grad_out = (2.0 * error).astype(jnp.bfloat16)
    attn_wide = widen(attn)
    grad_wide = widen(grad_out)
    weight_part = jnp.einsum('tf,td->fd', attn_wide, grad_wide)
    grad_attn = jnp.einsum('td,fd->tf', grad_wide, out_weight.astype(jnp.float32)).astype(jnp.bfloat16)
    grad_attn_wide = widen(grad_attn)
    delta = lax.optimization_barrier(jnp.sum((grad_attn_wide * attn_wide).reshape(SEQ, HEADS, HEAD_DIM), axis=2)).T
    back_probs = jnp.where(allowed, jnp.exp(masked - log_norm[:, :, None]), 0.0)
    grad_heads = grad_attn_wide.reshape(SEQ, HEADS, HEAD_DIM)
    dprobs = jnp.einsum('qhe,khe->hqk', grad_heads, value_heads)
    dscores = widen((back_probs * (dprobs - delta[:, :, None])).astype(jnp.bfloat16))
    query_raw = jnp.einsum('hqk,khe->qhe', dscores, key_heads) * score_scale
    key_raw = jnp.einsum('hqk,qhe->khe', dscores, query_heads) * score_scale
    back_weights = widen(back_probs.astype(jnp.bfloat16))
    value_raw = jnp.einsum('hqk,qhe->khe', back_weights, grad_heads)
    return (query_raw.reshape(SEQ, FEAT), key_raw.reshape(SEQ, FEAT), value_raw.reshape(SEQ, FEAT), weight_part, jnp.sum(error * error))

def reference(query_rows, key_rows, value_rows, out_weight, target, lengths, segments):

    def per_sample(packed):
        return one_sample(packed, out_weight)
    results = lax.map(per_sample, (query_rows, key_rows, value_rows, target, lengths, segments))
    count = jnp.sum(lengths).astype(jnp.float32)
    ratio = jnp.float32(SAMPLES * SEQ) / count
    query_grad = ratio * results[0]
    key_grad = ratio * results[1]
    value_grad = ratio * results[2]
    weight_grad = lax.optimization_barrier(jnp.sum(results[3], axis=0)) * (ratio / SEQ)
    loss = jnp.sum(results[4]) / (count * WIDTH)
    return (query_grad, key_grad, value_grad, weight_grad, loss)
```

```python
import functools
import math

import jax
import jax.numpy as jnp
from jax import lax
from jax.experimental import pallas as pl
from jax.experimental.pallas import tpu as pltpu
from jax.sharding import PartitionSpec as P

MESH = pl.DeviceIdType.MESH
WIDTH = 1152
HEADS = 8
HEAD_DIM = 72
FEAT = 576
PAIRS = HEADS // 2
NEG_LARGE = -1e30
F32 = jnp.float32
BF16 = jnp.bfloat16
KEY, VALUE, QUERY, GRAD = range(4)


def window(pair):
    low = (2 * HEAD_DIM * pair) // 128 * 128
    return low, min(low + 256, FEAT)


def lane_mask(head, low, high):
    lane = low + lax.broadcasted_iota(jnp.int32, (1, high - low), 1)
    first = head * HEAD_DIM
    return ((lane >= first) & (lane < first + HEAD_DIM)).astype(F32)


def nt(left, right):
    return lax.dot_general(left, right, (((1,), (1,)), ((), ())), preferred_element_type=F32)


def nn(left, right):
    return lax.dot_general(left, right, (((1,), (0,)), ((), ())), preferred_element_type=F32)


def tn(left, right):
    return lax.dot_general(left, right, (((0,), (0,)), ((), ())), preferred_element_type=F32)


def kernel(
    members,
    groups,
    len_ref,
    seg_ref,
    q_ref,
    k_ref,
    v_ref,
    w_hbm,
    t_hbm,
    dq_ref,
    dk_ref,
    dv_ref,
    dw_ref,
    loss_ref,
    w_ref,
    t_ref,
    all_ref,
    seg_own,
    seg_all,
    stat_own,
    stat_all,
    stat_rows,
    bias_ref,
    prob_ref,
    attn_ref,
    dout_ref,
    part_ref,
    w1_ref,
    keep_ref,
    wx_ref,
    w2_ref,
    wz_ref,
    w3_ref,
    fin_ref,
    w4_ref,
    tile_own,
    tile_all,
    sum_own,
    sum_all,
    load_sem,
    send_sem,
    recv_sem,
    seg_send,
    seg_recv,
    stat_send,
    stat_recv,
    tile_send,
    tile_recv,
    sum_send,
    sum_recv,
    s1,
    r1,
    s2,
    r2,
    s3,
    r3,
    s4,
    r4,
):
    rows = q_ref.shape[0]
    total = rows * members
    chips = members // 2
    half = groups // 2
    outer = groups // 2
    mine = outer // 2
    me = lax.axis_index("patch")
    dp = lax.axis_index("dp")
    chip, core = me // 2, me % 2
    step_a, step_b = dp // 2, dp % 2
    partner = chip * 2 + 1 - core

    def patch_peer(shift):
        return lax.rem(me + shift, members)

    def dp_peer(shift):
        return lax.rem(dp + shift, groups)

    def far(shift):
        return lax.rem(chip + shift, chips)

    loads = [
        pltpu.make_async_copy(w_hbm, w_ref, load_sem.at[0]),
        pltpu.make_async_copy(t_hbm, t_ref, load_sem.at[1]),
    ]
    for load in loads:
        load.start()

    barrier = pltpu.get_barrier_semaphore()
    for shift in range(1, members):
        pl.semaphore_signal(barrier, inc=1, device_id=(dp, patch_peer(shift)), device_id_type=MESH)
    for shift in range(1, groups):
        pl.semaphore_signal(barrier, inc=1, device_id=(dp_peer(shift), me), device_id_type=MESH)
    seg_own[...] = jnp.broadcast_to(seg_ref[...], seg_own.shape)
    pl.semaphore_wait(barrier, members + groups - 2)

    def copy(src, dst, send, recv, device):
        return pltpu.make_async_remote_copy(
            src_ref=src, dst_ref=dst, send_sem=send, recv_sem=recv, device_id=device, device_id_type=MESH
        )

    pending = []

    def start(item):
        item.start()
        pending.append(item)

    def spread(array, src):
        dst = all_ref.at[array, me]
        for shift in range(1, chips):
            start(copy(src, dst, send_sem.at[array, shift], recv_sem.at[array, me], (dp, far(shift) * 2 + core)))
        start(copy(src, dst, send_sem.at[array, 0], recv_sem.at[array, me], (dp, partner)))

    def arrived(array, owner):
        slot = all_ref.at[array, owner]
        return copy(slot, slot, send_sem.at[array, 0], recv_sem.at[array, owner], (dp, partner)).wait_recv()

    def relay(array):
        for shift in range(1, chips):
            owner = far(shift) * 2 + core
            arrived(array, owner)
            slot = all_ref.at[array, owner]
            start(copy(slot, slot, send_sem.at[array, chips - 1 + shift], recv_sem.at[array, owner], (dp, partner)))

    def finish(array):
        arrived(array, partner)
        for shift in range(1, chips):
            arrived(array, far(shift) * 2 + 1 - core)

    def small(own, everyone, send, recv):
        for shift in range(1, members):
            start(copy(own, everyone.at[me], send.at[shift], recv.at[me], (dp, patch_peer(shift))))

    def small_wait(own, everyone, send, recv):
        for shift in range(1, members):
            owner = patch_peer(shift)
            copy(own, everyone.at[owner], send.at[shift], recv.at[owner], (dp, owner)).wait_recv()

    small(seg_own, seg_all, seg_send, seg_recv)
    spread(KEY, k_ref)
    spread(VALUE, v_ref)
    spread(QUERY, q_ref)
    all_ref[KEY, me] = k_ref[...]
    all_ref[VALUE, me] = v_ref[...]
    all_ref[QUERY, me] = q_ref[...]
    seg_all[me] = seg_own[...]

    masks = [
        [lane_mask(2 * pair + side, *window(pair)) for side in (0, 1)] for pair in range(PAIRS)
    ]

    def stacked(value, pair):
        low, high = window(pair)
        part = value[:, low:high]
        return jnp.concatenate(
            [part * masks[pair][0].astype(BF16), part * masks[pair][1].astype(BF16)], axis=0
        )

    def merged(value, pair):
        return value[:rows] * masks[pair][0] + value[rows:] * masks[pair][1]

    def whole(array, pair):
        low, high = window(pair)
        return all_ref[array, :, :, low:high].reshape(total, high - low)

    def put(out_ref, value, pair):
        low, high = window(pair)
        if pair == 0:
            out_ref[:, low:high] = value
        else:
            previous = window(pair - 1)[1]
            out_ref[:, low:previous] += value[:, : previous - low]
            out_ref[:, previous:high] = value[:, previous - low :]

    length = len_ref[0]
    small_wait(seg_own, seg_all, seg_send, seg_recv)
    seg_row = jnp.concatenate([seg_all[j][0:1] for j in range(members)], axis=1)
    position = lax.broadcasted_iota(jnp.int32, (1, total), 1)
    group_row = jnp.where(position < length, seg_row, -1).astype(F32)
    own_position = me * rows + lax.broadcasted_iota(jnp.int32, (rows, 1), 0)
    own_live = own_position < length
    wide_own = jnp.broadcast_to(seg_own[0:1].astype(F32), (rows, rows)).T
    own_column = jnp.where(own_live, wide_own[:, 0:1], -1.0)
    bias_ref[...] = jnp.where(own_column == group_row, 0.0, NEG_LARGE)

    log_scale = math.log2(math.e) / math.sqrt(HEAD_DIM)
    score_scale = 1.0 / math.sqrt(HEAD_DIM)

    def biased(scores):
        bias = bias_ref[...]
        return jnp.concatenate([scores[:rows] * log_scale + bias, scores[rows:] * log_scale + bias], axis=0)

    relay(KEY)
    finish(KEY)
    stats = []
    for pair in range(PAIRS):
        scores = biased(nt(stacked(q_ref[...], pair), whole(KEY, pair)))
        row_max = jnp.max(scores, axis=1, keepdims=True)
        probs = jnp.exp2(scores - row_max)
        denom = jnp.sum(probs, axis=1, keepdims=True)
        prob_ref[pair] = probs
        stats.append((row_max + jnp.log2(denom), denom))
    relay(VALUE)
    finish(VALUE)
    for pair in range(PAIRS):
        accum = nn(prob_ref[pair].astype(BF16), whole(VALUE, pair))
        put(attn_ref, merged(accum / stats[pair][1], pair), pair)
    attn_wide = attn_ref[...]
    attn = attn_wide.astype(BF16)
    loads[0].wait()
    loads[1].wait()
    output = nn(attn, w_ref[...])
    error = jnp.where(own_live, output - t_ref[...].astype(F32), 0.0)
    loss_part = jnp.sum(jnp.sum(error * error, axis=0, keepdims=True), axis=1, keepdims=True)
    tile_own[...] = jnp.broadcast_to(loss_part, tile_own.shape)
    dout_ref[...] = (2.0 * error).astype(BF16)
    grad_attn = nt(dout_ref[...], w_ref[...]).astype(BF16)
    all_ref[GRAD, me] = grad_attn
    relay(QUERY)
    spread(GRAD, all_ref.at[GRAD, me])
    small(tile_own, tile_all, tile_send, tile_recv)

    product = grad_attn.astype(F32) * attn.astype(F32)
    lane = lax.broadcasted_iota(jnp.int32, (rows, 128), 1)
    stat = jnp.zeros((rows, 128), F32)
    deltas = []
    for pair in range(PAIRS):
        low, high = window(pair)
        for side in (0, 1):
            head = 2 * pair + side
            delta = jnp.sum(product[:, low:high] * masks[pair][side], axis=1, keepdims=True)
            deltas.append(delta)
            log_norm = stats[pair][0][side * rows : (side + 1) * rows]
            stat = jnp.where(lane == head, log_norm, stat)
            stat = jnp.where(lane == HEADS + head, delta, stat)
    stat_own[...] = stat.T[: 2 * HEADS]
    small(stat_own, stat_all, stat_send, stat_recv)
    stat_all[me] = stat_own[...]

    share = WIDTH // groups
    part = tn(dout_ref[...], attn)
    for block in range(groups):
        part_ref[block] = part[block * share : (block + 1) * share].astype(BF16)
    first = core * half
    other = (1 - core) * half
    stage1 = copy(part_ref.at[pl.ds(other, half)], w1_ref, s1, r1, (dp, partner))
    start(stage1)

    def query_pass(pair):
        delta = jnp.concatenate([deltas[2 * pair], deltas[2 * pair + 1]], axis=0)
        dprobs = nt(stacked(grad_attn, pair), whole(VALUE, pair))
        dscores = prob_ref[pair] * (1.0 / stats[pair][1]) * (dprobs - delta)
        value = nn(dscores.astype(BF16), whole(KEY, pair))
        put(dq_ref, merged(value, pair) * score_scale, pair)

    query_pass(0)
    query_pass(1)

    stage1.wait_recv()
    stage2 = []
    for i in range(mine):
        away = 2 * i + 1 - step_b
        near = 2 * i + step_b
        wx_ref[i] = (part_ref[first + away].astype(F32) + w1_ref[away].astype(F32)).astype(BF16)
        item = copy(wx_ref.at[i], w2_ref.at[i], s2.at[i], r2.at[i], (step_a * 2 + 1 - step_b, me))
        start(item)
        stage2.append(item)
        keep_ref[i] = part_ref[first + near].astype(F32) + w1_ref[near].astype(F32)

    relay(GRAD)
    query_pass(2)
    query_pass(3)
    finish(QUERY)
    finish(GRAD)
    small_wait(stat_own, stat_all, stat_send, stat_recv)
    stat_rows[...] = jnp.concatenate([stat_all[j] for j in range(members)], axis=1)

    def key_pass(pair):
        def spread_rows(base):
            return jnp.concatenate(
                [
                    jnp.broadcast_to(stat_rows[base + 2 * pair + side : base + 2 * pair + side + 1, :], (rows, total))
                    for side in (0, 1)
                ],
                axis=0,
            )

        queries = whole(QUERY, pair)
        grads = whole(GRAD, pair)
        scores = biased(nt(stacked(k_ref[...], pair), queries))
        probs = jnp.exp2(scores - spread_rows(0))
        put(dv_ref, merged(nn(probs.astype(BF16), grads), pair), pair)
        dprobs = nt(stacked(v_ref[...], pair), grads)
        dscores = (probs * (dprobs - spread_rows(HEADS))).astype(BF16)
        put(dk_ref, merged(nn(dscores, queries), pair) * score_scale, pair)

    def third(i):
        stage2[i].wait_recv()
        wz_ref[i] = (keep_ref[i] + w2_ref[i].astype(F32)).astype(BF16)
        owner = core * mine + i
        item = copy(wz_ref.at[i], w3_ref.at[step_a], s3.at[i], r3.at[step_a], (owner * 2 + step_b, me))

        @pl.when(owner != step_a)
        def _():
            item.start()

        return owner, item

    key_pass(0)
    stage3 = [third(0)]
    key_pass(1)
    stage3 += [third(i) for i in range(1, mine)]

    small_wait(tile_own, tile_all, tile_send, tile_recv)
    tile_all[me] = tile_own[...]
    pack_loss = tile_all[0]
    for j in range(1, members):
        pack_loss = pack_loss + tile_all[j]
    tile_lane = lax.broadcasted_iota(jnp.int32, pack_loss.shape, 1)
    sum_own[...] = jnp.where(tile_lane == 0, pack_loss, length.astype(F32))
    for shift in range(1, groups):
        start(copy(sum_own, sum_all.at[dp], sum_send.at[shift], sum_recv.at[dp], (dp_peer(shift), me)))
    sum_all[dp] = sum_own[...]

    key_pass(2)

    collect = step_a // mine
    is_collector = core == collect
    stage4 = [
        copy(fin_ref, w4_ref.at[chip], s4.at[shift], r4.at[chip], (dp, patch_peer(shift)))
        for shift in range(1, members)
    ]

    @pl.when(is_collector)
    def _():
        summed = wz_ref[step_a - core * mine].astype(F32)
        for shift in range(1, outer):
            source = lax.rem(step_a + shift, outer)
            copy(wz_ref.at[0], w3_ref.at[source], s3.at[0], r3.at[source], (source * 2 + step_b, me)).wait_recv()
            summed = summed + w3_ref[source].astype(F32)
        fin_ref[...] = summed.astype(BF16)
        for item in stage4:
            item.start()
        w4_ref[chip] = fin_ref[...]

    key_pass(3)

    for shift in range(1, groups):
        source = dp_peer(shift)
        copy(sum_own, sum_all.at[source], sum_send.at[shift], sum_recv.at[source], (source, me)).wait_recv()
    totals = sum_all[0]
    for j in range(1, groups):
        totals = totals + sum_all[j]
    count = totals[0:1, 1:2]
    ratio = (groups * total) / count
    loss_ref[...] = jnp.broadcast_to(totals[0:1, 0:1] / (count * WIDTH), loss_ref.shape)
    dq_ref[...] = dq_ref[...] * ratio
    dk_ref[...] = dk_ref[...] * ratio
    dv_ref[...] = dv_ref[...] * ratio

    def fetched(owner):
        copy(fin_ref, w4_ref.at[owner], s4.at[0], r4.at[owner], (dp, partner)).wait_recv()

    @pl.when(jnp.logical_not(is_collector))
    def _():
        fetched(chip)

    for shift in range(1, chips):
        fetched(far(shift))
    features = dw_ref.shape[0]
    chosen = (
        lax.broadcasted_iota(jnp.int32, (features, FEAT), 1)
        == me * features + lax.broadcasted_iota(jnp.int32, (features, FEAT), 0)
    ).astype(F32).astype(BF16)
    result = nt(chosen, w4_ref[0])
    for j in range(1, chips):
        result = result + nt(chosen, w4_ref[j])
    dw_ref[...] = result * (ratio / total)

    for item in pending:
        item.wait_send()
    for owner, item in stage3:

        @pl.when(owner != step_a)
        def _():
            item.wait_send()

    @pl.when(is_collector)
    def _():
        for item in stage4:
            item.wait_send()


def solution(mesh):
    members, groups = mesh.shape["patch"], mesh.shape["dp"]

    def local(query_rows, key_rows, value_rows, out_weight, target, lengths, segments):
        rows = query_rows.shape[1]
        total = rows * members
        chips = members // 2
        outer = groups // 2
        mine = outer // 2
        share = WIDTH // groups
        vmem = pl.BlockSpec(memory_space=pltpu.VMEM)
        hbm = pl.BlockSpec(memory_space=pl.ANY)
        dma = pltpu.SemaphoreType.DMA
        outs = pl.pallas_call(
            functools.partial(kernel, members, groups),
            out_shape=(
                jax.ShapeDtypeStruct((rows, FEAT), F32),
                jax.ShapeDtypeStruct((rows, FEAT), F32),
                jax.ShapeDtypeStruct((rows, FEAT), F32),
                jax.ShapeDtypeStruct((FEAT // members, share), F32),
                jax.ShapeDtypeStruct((8, 128), F32),
            ),
            in_specs=[pl.BlockSpec(memory_space=pltpu.SMEM), vmem, vmem, vmem, vmem, hbm, hbm],
            out_specs=(vmem,) * 5,
            scratch_shapes=[
                pltpu.VMEM((FEAT, WIDTH), BF16),
                pltpu.VMEM((rows, WIDTH), BF16),
                pltpu.VMEM((4, members, rows, FEAT), BF16),
                pltpu.VMEM((8, rows), jnp.int32),
                pltpu.VMEM((members, 8, rows), jnp.int32),
                pltpu.VMEM((2 * HEADS, rows), F32),
                pltpu.VMEM((members, 2 * HEADS, rows), F32),
                pltpu.VMEM((2 * HEADS, total), F32),
                pltpu.VMEM((rows, total), F32),
                pltpu.VMEM((PAIRS, 2 * rows, total), F32),
                pltpu.VMEM((rows, FEAT), F32),
                pltpu.VMEM((rows, WIDTH), BF16),
                pltpu.VMEM((groups, share, FEAT), BF16),
                pltpu.VMEM((groups // 2, share, FEAT), BF16),
                pltpu.VMEM((mine, share, FEAT), F32),
                pltpu.VMEM((mine, share, FEAT), BF16),
                pltpu.VMEM((mine, share, FEAT), BF16),
                pltpu.VMEM((mine, share, FEAT), BF16),
                pltpu.VMEM((outer, share, FEAT), BF16),
                pltpu.VMEM((share, FEAT), BF16),
                pltpu.VMEM((chips, share, FEAT), BF16),
                pltpu.VMEM((8, 128), F32),
                pltpu.VMEM((members, 8, 128), F32),
                pltpu.VMEM((8, 128), F32),
                pltpu.VMEM((groups, 8, 128), F32),
                dma((2,)),
                dma((4, members)),
                dma((4, members)),
                dma((members,)),
                dma((members,)),
                dma((members,)),
                dma((members,)),
                dma((members,)),
                dma((members,)),
                dma((groups,)),
                dma((groups,)),
                dma,
                dma,
                dma((mine,)),
                dma((mine,)),
                dma((mine,)),
                dma((outer,)),
                dma((members,)),
                dma((chips,)),
            ],
            compiler_params=pltpu.CompilerParams(collective_id=0, has_side_effects=True),
            name="sublayer",
        )(lengths, segments, query_rows[0], key_rows[0], value_rows[0], out_weight, target[0])
        return (outs[0][None], outs[1][None], outs[2][None], outs[3], outs[4][0, 0])

    placed = (
        P("dp", "patch", None),
        P("dp", "patch", None),
        P("dp", "patch", None),
        P(),
        P("dp", "patch", None),
        P("dp"),
        P("dp", "patch"),
    )
    return jax.shard_map(
        local,
        mesh=mesh,
        in_specs=placed,
        out_specs=(
            P("dp", "patch", None),
            P("dp", "patch", None),
            P("dp", "patch", None),
            P("patch", "dp"),
            P(),
        ),
        check_vma=False,
    )
```

```python
import functools
import math

import jax
import jax.numpy as jnp
from jax import lax
from jax.experimental import pallas as pl
from jax.experimental.pallas import tpu as pltpu
from jax.sharding import PartitionSpec as P

MESH = pl.DeviceIdType.MESH
WIDTH = 1152
HEADS = 8
HEAD_DIM = 72
FEAT = 576
PAIRS = HEADS // 2
PAIR_ROWS = 2 * HEAD_DIM
FEAT_PAD = 640
SPAN = 256
NEG_LARGE = -1e30
F32 = jnp.float32
BF16 = jnp.bfloat16
KEY, VALUE, QUERY, GRAD = range(4)


def nt(left, right):
    return lax.dot_general(left, right, (((1,), (1,)), ((), ())), preferred_element_type=F32)


def nn(left, right):
    return lax.dot_general(left, right, (((1,), (0,)), ((), ())), preferred_element_type=F32)


def tn(left, right):
    return lax.dot_general(left, right, (((0,), (0,)), ((), ())), preferred_element_type=F32)


def span_start(owner, features):
    return pl.multiple_of(jnp.minimum(owner * features // 128 * 128, FEAT_PAD - SPAN), 128)


def kernel(
    members,
    groups,
    len_ref,
    seg_ref,
    q_ref,
    k_ref,
    v_ref,
    w_hbm,
    t_hbm,
    dq_ref,
    dk_ref,
    dv_ref,
    dw_ref,
    sum_ref,
    w_ref,
    t_ref,
    seg_row_ref,
    all_ref,
    seg_own,
    seg_all,
    stat_own,
    stat_all,
    stat_columns,
    bias_ref,
    prob_ref,
    attn_ref,
    dout_ref,
    part_ref,
    w1_ref,
    keep_ref,
    wx_ref,
    w2_ref,
    wz_ref,
    w3_ref,
    fin_ref,
    w4_ref,
    tile_own,
    tile_all,
    sum_own,
    sum_all,
    load_sem,
    send_sem,
    recv_sem,
    seg_send,
    seg_recv,
    stat_send,
    stat_recv,
    tile_send,
    tile_recv,
    sum_send,
    sum_recv,
    s1,
    r1,
    s2,
    r2,
    s3,
    r3,
    s4,
    r4,
):
    rows = q_ref.shape[1]
    total = rows * members
    chips = members // 2
    half = groups // 2
    outer = groups // 2
    mine = outer // 2
    features = dw_ref.shape[0]
    me = lax.axis_index("patch")
    dp = lax.axis_index("dp")
    chip, core = me // 2, me % 2
    step_a, step_b = dp // 2, dp % 2
    partner = chip * 2 + 1 - core

    def patch_peer(shift):
        return lax.rem(me + shift, members)

    def dp_peer(shift):
        return lax.rem(dp + shift, groups)

    def far(shift):
        return lax.rem(chip + shift, chips)

    loads = [
        pltpu.make_async_copy(seg_ref, seg_row_ref, load_sem.at[0]),
        pltpu.make_async_copy(k_ref, all_ref.at[KEY, me], load_sem.at[1]),
        pltpu.make_async_copy(v_ref, all_ref.at[VALUE, me], load_sem.at[2]),
        pltpu.make_async_copy(q_ref, all_ref.at[QUERY, me], load_sem.at[3]),
        pltpu.make_async_copy(w_hbm, w_ref, load_sem.at[4]),
        pltpu.make_async_copy(t_hbm, t_ref, load_sem.at[5]),
    ]
    for load in loads:
        load.start()

    barrier = pltpu.get_barrier_semaphore()
    for shift in range(1, members):
        pl.semaphore_signal(barrier, inc=1, device_id=(dp, patch_peer(shift)), device_id_type=MESH)
    for shift in range(1, groups):
        pl.semaphore_signal(barrier, inc=1, device_id=(dp_peer(shift), me), device_id_type=MESH)
    loads[0].wait()
    seg_own[...] = jnp.broadcast_to(seg_row_ref[...], seg_own.shape)
    seg_all[me] = seg_own[...]
    for load in loads[1:4]:
        load.wait()
    pl.semaphore_wait(barrier, members + groups - 2)

    def copy(src, dst, send, recv, device):
        return pltpu.make_async_remote_copy(
            src_ref=src, dst_ref=dst, send_sem=send, recv_sem=recv, device_id=device, device_id_type=MESH
        )

    pending = []

    def start(item):
        item.start()
        pending.append(item)

    def rows_of(pair):
        return pl.ds(PAIR_ROWS * pair, PAIR_ROWS)

    def spread(array, pair):
        src = dst = all_ref.at[array, me, rows_of(pair)]
        recv = recv_sem.at[array, me, pair]
        for shift in range(1, chips):
            start(copy(src, dst, send_sem.at[array, shift, pair], recv, (dp, far(shift) * 2 + core)))
        start(copy(src, dst, send_sem.at[array, 0, pair], recv, (dp, partner)))

    def arrived(array, owner, pair):
        slot = all_ref.at[array, owner, rows_of(pair)]
        copy(slot, slot, send_sem.at[array, 0, pair], recv_sem.at[array, owner, pair], (dp, partner)).wait_recv()

    def relay(array, pair):
        for shift in range(1, chips):
            owner = far(shift) * 2 + core
            arrived(array, owner, pair)
            slot = all_ref.at[array, owner, rows_of(pair)]
            send = send_sem.at[array, chips - 1 + shift, pair]
            start(copy(slot, slot, send, recv_sem.at[array, owner, pair], (dp, partner)))

    def finish(array, pair):
        arrived(array, partner, pair)
        for shift in range(1, chips):
            arrived(array, far(shift) * 2 + 1 - core, pair)

    def small(own, everyone, send, recv):
        for shift in range(1, members):
            start(copy(own, everyone.at[me], send.at[shift], recv.at[me], (dp, patch_peer(shift))))

    def small_wait(own, everyone, send, recv):
        for shift in range(1, members):
            owner = patch_peer(shift)
            copy(own, everyone.at[owner], send.at[shift], recv.at[owner], (dp, owner)).wait_recv()

    small(seg_own, seg_all, seg_send, seg_recv)
    for pair in range(PAIRS):
        spread(KEY, pair)
        spread(VALUE, pair)
    for pair in range(PAIRS):
        spread(QUERY, pair)

    upper = lax.broadcasted_iota(jnp.int32, (PAIR_ROWS, 1), 0) < HEAD_DIM
    masks = [upper.astype(F32).astype(BF16), jnp.logical_not(upper).astype(F32).astype(BF16)]

    def stacked(value):
        return jnp.concatenate([value * masks[0], value * masks[1]], axis=1)

    def merged(value):
        return jnp.concatenate([value[:HEAD_DIM, :rows], value[HEAD_DIM:, rows:]], axis=0)

    def part_of(ref, pair):
        return ref[PAIR_ROWS * pair : PAIR_ROWS * (pair + 1), :]

    def own(array, pair):
        return all_ref[array, me, PAIR_ROWS * pair : PAIR_ROWS * (pair + 1), :]

    def whole(array, pair):
        low = PAIR_ROWS * pair
        return jnp.concatenate([all_ref[array, j, low : low + PAIR_ROWS, :] for j in range(members)], axis=1)

    length = len_ref[0]
    lane_position = lax.broadcasted_iota(jnp.int32, (1, rows), 1)
    own_live = me * rows + lax.broadcasted_iota(jnp.int32, (rows, 1), 0) < length
    own_group = jnp.where(me * rows + lane_position < length, seg_own[0:1], -1).astype(F32)
    small_wait(seg_own, seg_all, seg_send, seg_recv)
    for j in range(members):
        group = jnp.where(j * rows + lane_position < length, seg_all[j][0:1], -1).astype(F32)
        group = jnp.broadcast_to(group, (rows, rows)).T
        bias_ref[j * rows : (j + 1) * rows, :] = jnp.where(group == own_group, 0.0, NEG_LARGE)
    attn_ref[FEAT:, :] = jnp.zeros((FEAT_PAD - FEAT, rows), F32)

    log_scale = math.log2(math.e) / math.sqrt(HEAD_DIM)
    score_scale = 1.0 / math.sqrt(HEAD_DIM)

    def biased(scores):
        bias = bias_ref[...]
        return scores * log_scale + jnp.concatenate([bias, bias], axis=1)

    denoms = []
    for pair in range(PAIRS):
        relay(KEY, pair)
        relay(VALUE, pair)
        finish(KEY, pair)
        scores = biased(tn(whole(KEY, pair), stacked(own(QUERY, pair))))
        row_max = jnp.max(scores, axis=0, keepdims=True)
        probs = jnp.exp2(scores - row_max)
        denom = jnp.sum(probs, axis=0, keepdims=True)
        prob_ref[pair] = probs
        log_norm = row_max + jnp.log2(denom)
        for side in (0, 1):
            head = 2 * pair + side
            stat_own[head : head + 1, :] = log_norm[:, side * rows : (side + 1) * rows]
        denoms.append(denom)
        finish(VALUE, pair)
        accum = nn(whole(VALUE, pair), probs.astype(BF16))
        attn_ref[PAIR_ROWS * pair : PAIR_ROWS * (pair + 1), :] = merged(accum / denom)

    attn = attn_ref[...].T.astype(BF16)
    loads[4].wait()
    loads[5].wait()
    output = nn(attn[:, :FEAT], w_ref[...])
    error = jnp.where(own_live, output - t_ref[...].astype(F32), 0.0)
    dout_ref[...] = (2.0 * error).astype(BF16)

    share = WIDTH // groups
    part = tn(dout_ref[...], attn)
    for block in range(groups):
        part_ref[block] = part[block * share : (block + 1) * share].astype(BF16)
    first = core * half
    other = (1 - core) * half
    stage1 = copy(part_ref.at[pl.ds(other, half)], w1_ref, s1, r1, (dp, partner))
    start(stage1)

    for pair in range(PAIRS):
        grad = nt(part_of(w_ref, pair), dout_ref[...]).astype(BF16)
        all_ref[GRAD, me, PAIR_ROWS * pair : PAIR_ROWS * (pair + 1), :] = grad
        spread(GRAD, pair)
        attn_pair = part_of(attn_ref, pair).astype(BF16).astype(F32)
        product = grad.astype(F32) * attn_pair
        for side in (0, 1):
            head = HEADS + 2 * pair + side
            stat_own[head : head + 1, :] = jnp.sum(
                product[HEAD_DIM * side : HEAD_DIM * (side + 1)], axis=0, keepdims=True
            )
    small(stat_own, stat_all, stat_send, stat_recv)
    stat_all[me] = stat_own[...]
    loss_part = jnp.sum(jnp.sum(error * error, axis=0, keepdims=True), axis=1, keepdims=True)
    tile_own[...] = jnp.broadcast_to(loss_part, tile_own.shape)
    small(tile_own, tile_all, tile_send, tile_recv)

    def query_pass(pair):
        low = HEADS + 2 * pair
        delta = jnp.concatenate([stat_own[low : low + 1, :], stat_own[low + 1 : low + 2, :]], axis=1)
        dprobs = tn(whole(VALUE, pair), stacked(own(GRAD, pair)))
        dscores = prob_ref[pair] * (1.0 / denoms[pair]) * (dprobs - delta)
        value = nn(whole(KEY, pair), dscores.astype(BF16))
        dq_ref[PAIR_ROWS * pair : PAIR_ROWS * (pair + 1), :] = merged(value) * score_scale

    stage1.wait_recv()
    stage2 = []
    for i in range(mine):
        away = 2 * i + 1 - step_b
        wx_ref[i] = (part_ref[first + away].astype(F32) + w1_ref[away].astype(F32)).astype(BF16)
        item = copy(wx_ref.at[i], w2_ref.at[i], s2.at[i], r2.at[i], (step_a * 2 + 1 - step_b, me))
        start(item)
        stage2.append(item)
    for i in range(mine):
        near = 2 * i + step_b
        keep_ref[i] = part_ref[first + near].astype(F32) + w1_ref[near].astype(F32)
    for pair in range(PAIRS):
        relay(QUERY, pair)

    query_pass(0)
    query_pass(1)
    relay(GRAD, 0)
    relay(GRAD, 1)
    small_wait(stat_own, stat_all, stat_send, stat_recv)
    for j in range(members):
        tall = jnp.concatenate([stat_all[j], jnp.zeros((128 - 2 * HEADS, rows), F32)], axis=0)
        stat_columns[j * rows : (j + 1) * rows, :] = tall.T

    def third(i):
        stage2[i].wait_recv()
        wz_ref[i] = (keep_ref[i] + w2_ref[i].astype(F32)).astype(BF16)
        owner = core * mine + i
        item = copy(wz_ref.at[i], w3_ref.at[step_a], s3.at[i], r3.at[step_a], (owner * 2 + step_b, me))

        @pl.when(owner != step_a)
        def _():
            item.start()

        return owner, item

    def key_pass(pair):
        def columns(base):
            low = base + 2 * pair
            return jnp.concatenate(
                [jnp.broadcast_to(stat_columns[:, low + side : low + side + 1], (total, rows)) for side in (0, 1)],
                axis=1,
            )

        finish(QUERY, pair)
        finish(GRAD, pair)
        queries = whole(QUERY, pair)
        grads = whole(GRAD, pair)
        scores = biased(tn(queries, stacked(own(KEY, pair))))
        probs = jnp.exp2(scores - columns(0))
        dv_ref[PAIR_ROWS * pair : PAIR_ROWS * (pair + 1), :] = merged(nn(grads, probs.astype(BF16)))
        dprobs = tn(grads, stacked(own(VALUE, pair)))
        dscores = (probs * (dprobs - columns(HEADS))).astype(BF16)
        dk_ref[PAIR_ROWS * pair : PAIR_ROWS * (pair + 1), :] = merged(nn(queries, dscores)) * score_scale

    stage3 = [third(0)]
    relay(GRAD, 2)
    relay(GRAD, 3)
    query_pass(2)
    stage3 += [third(i) for i in range(1, mine)]
    query_pass(3)

    small_wait(tile_own, tile_all, tile_send, tile_recv)
    tile_all[me] = tile_own[...]
    pack_loss = tile_all[0]
    for j in range(1, members):
        pack_loss = pack_loss + tile_all[j]
    tile_lane = lax.broadcasted_iota(jnp.int32, pack_loss.shape, 1)
    sum_own[...] = jnp.where(tile_lane == 0, pack_loss, length.astype(F32))
    for shift in range(1, groups):
        start(copy(sum_own, sum_all.at[dp], sum_send.at[shift], sum_recv.at[dp], (dp_peer(shift), me)))
    sum_all[dp] = sum_own[...]

    key_pass(0)
    key_pass(1)

    collect = step_a // mine
    is_collector = core == collect
    stage4 = []
    for shift in range(1, members):
        target = patch_peer(shift)
        span = fin_ref.at[:, pl.ds(span_start(target, features), SPAN)]
        stage4.append(copy(span, w4_ref.at[chip], s4.at[shift], r4.at[chip], (dp, target)))

    @pl.when(is_collector)
    def _():
        summed = wz_ref[step_a - core * mine].astype(F32)
        for shift in range(1, outer):
            source = lax.rem(step_a + shift, outer)
            copy(wz_ref.at[0], w3_ref.at[source], s3.at[0], r3.at[source], (source * 2 + step_b, me)).wait_recv()
            summed = summed + w3_ref[source].astype(F32)
        fin_ref[...] = summed.astype(BF16)
        for item in stage4:
            item.start()
        w4_ref[chip] = fin_ref[:, pl.ds(span_start(me, features), SPAN)]

    key_pass(2)
    key_pass(3)

    for shift in range(1, groups):
        source = dp_peer(shift)
        copy(sum_own, sum_all.at[source], sum_send.at[shift], sum_recv.at[source], (source, me)).wait_recv()
    totals = sum_all[0]
    for j in range(1, groups):
        totals = totals + sum_all[j]
    sum_ref[...] = totals

    def fetched(owner):
        copy(w4_ref.at[owner], w4_ref.at[owner], s4.at[0], r4.at[owner], (dp, partner)).wait_recv()

    @pl.when(jnp.logical_not(is_collector))
    def _():
        fetched(chip)

    for shift in range(1, chips):
        fetched(far(shift))
    shape = (features, SPAN)
    start_lane = me * features - span_start(me, features)
    chosen = (
        lax.broadcasted_iota(jnp.int32, shape, 1) == start_lane + lax.broadcasted_iota(jnp.int32, shape, 0)
    ).astype(F32).astype(BF16)
    result = nt(chosen, w4_ref[0])
    for j in range(1, chips):
        result = result + nt(chosen, w4_ref[j])
    dw_ref[...] = result

    for item in pending:
        item.wait_send()
    for owner, item in stage3:

        @pl.when(owner != step_a)
        def _():
            item.wait_send()

    @pl.when(is_collector)
    def _():
        for item in stage4:
            item.wait_send()


def scale_kernel(slots, total, sum_ref, dq_ref, dk_ref, dv_ref, dw_ref, query_ref, key_ref, value_ref, weight_ref, loss_ref):
    count = sum_ref[0:1, 1:2]
    ratio = slots / count
    query_ref[...] = dq_ref[...] * ratio
    key_ref[...] = dk_ref[...] * ratio
    value_ref[...] = dv_ref[...] * ratio
    weight_ref[...] = dw_ref[...] * (ratio / total)
    loss_ref[...] = sum_ref[0:1, 0:1] / (count * WIDTH)


def solution(mesh):
    members, groups = mesh.shape["patch"], mesh.shape["dp"]

    def local(query_rows, key_rows, value_rows, out_weight, target, lengths, segments):
        rows = query_rows.shape[1]
        total = rows * members
        chips = members // 2
        outer = groups // 2
        mine = outer // 2
        share = WIDTH // groups
        vmem = pl.BlockSpec(memory_space=pltpu.VMEM)
        hbm = pl.BlockSpec(memory_space=pltpu.HBM)
        dma = pltpu.SemaphoreType.DMA
        outs = pl.pallas_call(
            functools.partial(kernel, members, groups),
            out_shape=(
                jax.ShapeDtypeStruct((FEAT, rows), F32),
                jax.ShapeDtypeStruct((FEAT, rows), F32),
                jax.ShapeDtypeStruct((FEAT, rows), F32),
                jax.ShapeDtypeStruct((FEAT // members, share), F32),
                jax.ShapeDtypeStruct((8, 128), F32),
            ),
            in_specs=[pl.BlockSpec(memory_space=pltpu.SMEM)] + [hbm] * 6,
            out_specs=(vmem,) * 5,
            scratch_shapes=[
                pltpu.VMEM((FEAT, WIDTH), BF16),
                pltpu.VMEM((rows, WIDTH), BF16),
                pltpu.VMEM((1, rows), jnp.int32),
                pltpu.VMEM((4, members, FEAT, rows), BF16),
                pltpu.VMEM((8, rows), jnp.int32),
                pltpu.VMEM((members, 8, rows), jnp.int32),
                pltpu.VMEM((2 * HEADS, rows), F32),
                pltpu.VMEM((members, 2 * HEADS, rows), F32),
                pltpu.VMEM((total, 128), F32),
                pltpu.VMEM((total, rows), F32),
                pltpu.VMEM((PAIRS, total, 2 * rows), F32),
                pltpu.VMEM((FEAT_PAD, rows), F32),
                pltpu.VMEM((rows, WIDTH), BF16),
                pltpu.VMEM((groups, share, FEAT_PAD), BF16),
                pltpu.VMEM((groups // 2, share, FEAT_PAD), BF16),
                pltpu.VMEM((mine, share, FEAT_PAD), F32),
                pltpu.VMEM((mine, share, FEAT_PAD), BF16),
                pltpu.VMEM((mine, share, FEAT_PAD), BF16),
                pltpu.VMEM((mine, share, FEAT_PAD), BF16),
                pltpu.VMEM((outer, share, FEAT_PAD), BF16),
                pltpu.VMEM((share, FEAT_PAD), BF16),
                pltpu.VMEM((chips, share, SPAN), BF16),
                pltpu.VMEM((8, 128), F32),
                pltpu.VMEM((members, 8, 128), F32),
                pltpu.VMEM((8, 128), F32),
                pltpu.VMEM((groups, 8, 128), F32),
                dma((6,)),
                dma((4, members, PAIRS)),
                dma((4, members, PAIRS)),
                dma((members,)),
                dma((members,)),
                dma((members,)),
                dma((members,)),
                dma((members,)),
                dma((members,)),
                dma((groups,)),
                dma((groups,)),
                dma,
                dma,
                dma((mine,)),
                dma((mine,)),
                dma((mine,)),
                dma((outer,)),
                dma((members,)),
                dma((chips,)),
            ],
            compiler_params=pltpu.CompilerParams(collective_id=0, has_side_effects=True, vmem_limit_bytes=65900000),
            name="sublayer",
        )(
            lengths,
            segments,
            query_rows[0].T,
            key_rows[0].T,
            value_rows[0].T,
            out_weight,
            target[0],
        )
        final = pl.pallas_call(
            functools.partial(scale_kernel, groups * total, total),
            out_shape=(
                jax.ShapeDtypeStruct((FEAT, rows), F32),
                jax.ShapeDtypeStruct((FEAT, rows), F32),
                jax.ShapeDtypeStruct((FEAT, rows), F32),
                jax.ShapeDtypeStruct((FEAT // members, share), F32),
                jax.ShapeDtypeStruct((1, 1), F32),
            ),
            in_specs=[vmem] * 5,
            out_specs=(vmem,) * 5,
            compiler_params=pltpu.CompilerParams(vmem_limit_bytes=65900000),
            name="scale",
        )(outs[4], *outs[:4])
        return (final[0].T[None], final[1].T[None], final[2].T[None], final[3], final[4].reshape(()))

    placed = (
        P("dp", "patch", None),
        P("dp", "patch", None),
        P("dp", "patch", None),
        P(),
        P("dp", "patch", None),
        P("dp"),
        P("dp", "patch"),
    )
    return jax.shard_map(
        local,
        mesh=mesh,
        in_specs=placed,
        out_specs=(
            P("dp", "patch", None),
            P("dp", "patch", None),
            P("dp", "patch", None),
            P("patch", "dp"),
            P(),
        ),
        check_vma=False,
    )
```

```python
import functools
import math

import jax
import jax.numpy as jnp
from jax import lax
from jax.experimental import pallas as pl
from jax.experimental.pallas import tpu as pltpu
from jax.sharding import PartitionSpec as P

MESH = pl.DeviceIdType.MESH
WIDTH = 1152
HEADS = 8
HEAD_DIM = 72
FEAT = 576
PAIRS = HEADS // 2
PAIR_ROWS = 2 * HEAD_DIM
FEAT_PAD = 640
SPAN = 256
NEG_LARGE = -1e30
F32 = jnp.float32
BF16 = jnp.bfloat16
KEY, VALUE, QUERY, GRAD = range(4)


def nt(left, right):
    return lax.dot_general(left, right, (((1,), (1,)), ((), ())), preferred_element_type=F32)


def nn(left, right):
    return lax.dot_general(left, right, (((1,), (0,)), ((), ())), preferred_element_type=F32)


def tn(left, right):
    return lax.dot_general(left, right, (((0,), (0,)), ((), ())), preferred_element_type=F32)


def span_start(owner, features):
    return pl.multiple_of(jnp.minimum(owner * features // 128 * 128, FEAT_PAD - SPAN), 128)


def kernel(
    members,
    groups,
    len_ref,
    seg_ref,
    q_ref,
    k_ref,
    v_ref,
    w_hbm,
    t_hbm,
    dq_ref,
    dk_ref,
    dv_ref,
    dw_ref,
    sum_ref,
    w_ref,
    t_ref,
    seg_row_ref,
    all_ref,
    seg_own,
    seg_all,
    stat_own,
    stat_all,
    stat_columns,
    bias_ref,
    prob_ref,
    attn_ref,
    dout_ref,
    part_ref,
    w1_ref,
    keep_ref,
    wx_ref,
    w2_ref,
    wz_ref,
    w3_ref,
    fin_ref,
    w4_ref,
    tile_own,
    tile_all,
    sum_own,
    sum_all,
    load_sem,
    send_sem,
    recv_sem,
    seg_send,
    seg_recv,
    stat_send,
    stat_recv,
    tile_send,
    tile_recv,
    sum_send,
    sum_recv,
    s1,
    r1,
    s2,
    r2,
    s3,
    r3,
    s4,
    r4,
):
    rows = q_ref.shape[1]
    total = rows * members
    chips = members // 2
    half = groups // 2
    outer = groups // 2
    mine = outer // 2
    features = dw_ref.shape[0]
    me = lax.axis_index("patch")
    dp = lax.axis_index("dp")
    chip, core = me // 2, me % 2
    step_a, step_b = dp // 2, dp % 2
    partner = chip * 2 + 1 - core

    def patch_peer(shift):
        return lax.rem(me + shift, members)

    def dp_peer(shift):
        return lax.rem(dp + shift, groups)

    def far(shift):
        return lax.rem(chip + shift, chips)

    loads = [
        pltpu.make_async_copy(seg_ref, seg_row_ref, load_sem.at[0]),
        pltpu.make_async_copy(k_ref, all_ref.at[KEY, me], load_sem.at[1]),
        pltpu.make_async_copy(v_ref, all_ref.at[VALUE, me], load_sem.at[2]),
        pltpu.make_async_copy(q_ref, all_ref.at[QUERY, me], load_sem.at[3]),
        pltpu.make_async_copy(w_hbm, w_ref, load_sem.at[4]),
        pltpu.make_async_copy(t_hbm, t_ref, load_sem.at[5]),
    ]
    for load in loads:
        load.start()

    barrier = pltpu.get_barrier_semaphore()
    for shift in range(1, members):
        pl.semaphore_signal(barrier, inc=1, device_id=(dp, patch_peer(shift)), device_id_type=MESH)
    for shift in range(1, groups):
        pl.semaphore_signal(barrier, inc=1, device_id=(dp_peer(shift), me), device_id_type=MESH)
    loads[0].wait()
    seg_own[...] = jnp.broadcast_to(seg_row_ref[...], seg_own.shape)
    seg_all[me] = seg_own[...]
    for load in loads[1:4]:
        load.wait()
    pl.semaphore_wait(barrier, members + groups - 2)

    def copy(src, dst, send, recv, device):
        return pltpu.make_async_remote_copy(
            src_ref=src, dst_ref=dst, send_sem=send, recv_sem=recv, device_id=device, device_id_type=MESH
        )

    pending = []

    def start(item):
        item.start()
        pending.append(item)

    def rows_of(pair):
        return pl.ds(PAIR_ROWS * pair, PAIR_ROWS)

    def spread(array, pair):
        src = dst = all_ref.at[array, me, rows_of(pair)]
        recv = recv_sem.at[array, me, pair]
        for shift in range(1, chips):
            start(copy(src, dst, send_sem.at[array, shift, pair], recv, (dp, far(shift) * 2 + core)))
        start(copy(src, dst, send_sem.at[array, 0, pair], recv, (dp, partner)))

    def arrived(array, owner, pair):
        slot = all_ref.at[array, owner, rows_of(pair)]
        copy(slot, slot, send_sem.at[array, 0, pair], recv_sem.at[array, owner, pair], (dp, partner)).wait_recv()

    def relay(array, pair):
        for shift in range(1, chips):
            owner = far(shift) * 2 + core
            arrived(array, owner, pair)
            slot = all_ref.at[array, owner, rows_of(pair)]
            send = send_sem.at[array, chips - 1 + shift, pair]
            start(copy(slot, slot, send, recv_sem.at[array, owner, pair], (dp, partner)))

    def finish(array, pair):
        arrived(array, partner, pair)
        for shift in range(1, chips):
            arrived(array, far(shift) * 2 + 1 - core, pair)

    def small(own, everyone, send, recv):
        for shift in range(1, members):
            start(copy(own, everyone.at[me], send.at[shift], recv.at[me], (dp, patch_peer(shift))))

    def small_wait(own, everyone, send, recv):
        for shift in range(1, members):
            owner = patch_peer(shift)
            copy(own, everyone.at[owner], send.at[shift], recv.at[owner], (dp, owner)).wait_recv()

    small(seg_own, seg_all, seg_send, seg_recv)
    for pair in range(PAIRS):
        spread(KEY, pair)
        spread(VALUE, pair)
    for pair in range(PAIRS):
        spread(QUERY, pair)

    upper = lax.broadcasted_iota(jnp.int32, (PAIR_ROWS, 1), 0) < HEAD_DIM
    masks = [upper.astype(F32).astype(BF16), jnp.logical_not(upper).astype(F32).astype(BF16)]

    def stacked(value):
        return jnp.concatenate([value * masks[0], value * masks[1]], axis=1)

    def merged(value):
        return jnp.concatenate([value[:HEAD_DIM, :rows], value[HEAD_DIM:, rows:]], axis=0)

    def part_of(ref, pair):
        return ref[PAIR_ROWS * pair : PAIR_ROWS * (pair + 1), :]

    def own(array, pair):
        return all_ref[array, me, PAIR_ROWS * pair : PAIR_ROWS * (pair + 1), :]

    def whole(array, pair):
        low = PAIR_ROWS * pair
        return jnp.concatenate([all_ref[array, j, low : low + PAIR_ROWS, :] for j in range(members)], axis=1)

    length = len_ref[0]
    lane_position = lax.broadcasted_iota(jnp.int32, (1, rows), 1)
    own_live = me * rows + lax.broadcasted_iota(jnp.int32, (rows, 1), 0) < length
    own_group = jnp.where(me * rows + lane_position < length, seg_own[0:1], -1).astype(F32)
    small_wait(seg_own, seg_all, seg_send, seg_recv)
    for j in range(members):
        group = jnp.where(j * rows + lane_position < length, seg_all[j][0:1], -1).astype(F32)
        group = jnp.broadcast_to(group, (rows, rows)).T
        bias_ref[j * rows : (j + 1) * rows, :] = jnp.where(group == own_group, 0.0, NEG_LARGE)
    attn_ref[FEAT:, :] = jnp.zeros((FEAT_PAD - FEAT, rows), F32)

    log_scale = math.log2(math.e) / math.sqrt(HEAD_DIM)
    score_scale = 1.0 / math.sqrt(HEAD_DIM)

    def biased(scores):
        bias = bias_ref[...]
        return scores * log_scale + jnp.concatenate([bias, bias], axis=1)

    denoms = []
    for pair in range(PAIRS):
        relay(KEY, pair)
        relay(VALUE, pair)
        finish(KEY, pair)
        scores = biased(tn(whole(KEY, pair), stacked(own(QUERY, pair))))
        row_max = jnp.max(scores, axis=0, keepdims=True)
        probs = jnp.exp2(scores - row_max)
        denom = jnp.sum(probs, axis=0, keepdims=True)
        prob_ref[pair] = probs
        log_norm = row_max + jnp.log2(denom)
        for side in (0, 1):
            head = 2 * pair + side
            stat_own[head : head + 1, :] = log_norm[:, side * rows : (side + 1) * rows]
        denoms.append(denom)
        finish(VALUE, pair)
        accum = nn(whole(VALUE, pair), probs.astype(BF16))
        attn_ref[PAIR_ROWS * pair : PAIR_ROWS * (pair + 1), :] = merged(accum / denom)

    attn = attn_ref[...].T.astype(BF16)
    loads[4].wait()
    loads[5].wait()
    output = nn(attn[:, :FEAT], w_ref[...])
    error = jnp.where(own_live, output - t_ref[...].astype(F32), 0.0)
    dout_ref[...] = (2.0 * error).astype(BF16)

    share = WIDTH // groups
    part = tn(dout_ref[...], attn)
    for block in range(groups):
        part_ref[block] = part[block * share : (block + 1) * share].astype(BF16)
    first = core * half
    other = (1 - core) * half
    stage1 = copy(part_ref.at[pl.ds(other, half)], w1_ref, s1, r1, (dp, partner))
    start(stage1)

    for pair in range(PAIRS):
        grad = nt(part_of(w_ref, pair), dout_ref[...]).astype(BF16)
        all_ref[GRAD, me, PAIR_ROWS * pair : PAIR_ROWS * (pair + 1), :] = grad
        spread(GRAD, pair)
        attn_pair = part_of(attn_ref, pair).astype(BF16).astype(F32)
        product = grad.astype(F32) * attn_pair
        for side in (0, 1):
            head = HEADS + 2 * pair + side
            stat_own[head : head + 1, :] = jnp.sum(
                product[HEAD_DIM * side : HEAD_DIM * (side + 1)], axis=0, keepdims=True
            )
    small(stat_own, stat_all, stat_send, stat_recv)
    stat_all[me] = stat_own[...]
    loss_part = jnp.sum(jnp.sum(error * error, axis=0, keepdims=True), axis=1, keepdims=True)
    tile_own[...] = jnp.broadcast_to(loss_part, tile_own.shape)
    small(tile_own, tile_all, tile_send, tile_recv)

    def query_pass(pair):
        low = HEADS + 2 * pair
        delta = jnp.concatenate([stat_own[low : low + 1, :], stat_own[low + 1 : low + 2, :]], axis=1)
        dprobs = tn(whole(VALUE, pair), stacked(own(GRAD, pair)))
        dscores = prob_ref[pair] * (1.0 / denoms[pair]) * (dprobs - delta)
        value = nn(whole(KEY, pair), dscores.astype(BF16))
        dq_ref[PAIR_ROWS * pair : PAIR_ROWS * (pair + 1), :] = merged(value) * score_scale

    stage1.wait_recv()
    cut = -(-share // 32) * 16
    pieces = [(i, side) for i in range(mine) for side in (0, 1)]
    spans = [pl.ds(0, cut), pl.ds(cut, share - cut)]
    stage2 = {}
    for i, side in pieces:
        away, span = 2 * i + 1 - step_b, spans[side]
        wx_ref[i, span] = (part_ref[first + away, span].astype(F32) + w1_ref[away, span].astype(F32)).astype(BF16)
        item = copy(
            wx_ref.at[i, span],
            w2_ref.at[i, span],
            s2.at[i, side],
            r2.at[i, side],
            (step_a * 2 + 1 - step_b, me),
        )
        start(item)
        stage2[i, side] = item
    for i in range(mine):
        near = 2 * i + step_b
        keep_ref[i] = part_ref[first + near].astype(F32) + w1_ref[near].astype(F32)
    for pair in range(PAIRS):
        relay(QUERY, pair)

    query_pass(0)
    relay(GRAD, 0)
    relay(GRAD, 1)
    small_wait(stat_own, stat_all, stat_send, stat_recv)
    for j in range(members):
        tall = jnp.concatenate([stat_all[j], jnp.zeros((128 - 2 * HEADS, rows), F32)], axis=0)
        stat_columns[j * rows : (j + 1) * rows, :] = tall.T

    def third(i, side):
        span = spans[side]
        stage2[i, side].wait_recv()
        wz_ref[i, span] = (keep_ref[i, span] + w2_ref[i, span].astype(F32)).astype(BF16)
        owner = core * mine + i
        item = copy(
            wz_ref.at[i, span],
            w3_ref.at[step_a, span],
            s3.at[i, side],
            r3.at[step_a, side],
            (owner * 2 + step_b, me),
        )

        @pl.when(owner != step_a)
        def _():
            item.start()

        return owner, item

    def key_pass(pair):
        def columns(base):
            low = base + 2 * pair
            return jnp.concatenate(
                [jnp.broadcast_to(stat_columns[:, low + side : low + side + 1], (total, rows)) for side in (0, 1)],
                axis=1,
            )

        finish(QUERY, pair)
        finish(GRAD, pair)
        queries = whole(QUERY, pair)
        grads = whole(GRAD, pair)
        scores = biased(tn(queries, stacked(own(KEY, pair))))
        probs = jnp.exp2(scores - columns(0))
        dv_ref[PAIR_ROWS * pair : PAIR_ROWS * (pair + 1), :] = merged(nn(grads, probs.astype(BF16)))
        dprobs = tn(grads, stacked(own(VALUE, pair)))
        dscores = (probs * (dprobs - columns(HEADS))).astype(BF16)
        dk_ref[PAIR_ROWS * pair : PAIR_ROWS * (pair + 1), :] = merged(nn(queries, dscores)) * score_scale

    stage3 = [third(*pieces[0])]
    relay(GRAD, 2)
    relay(GRAD, 3)
    query_pass(1)
    stage3.append(third(*pieces[1]))
    query_pass(2)
    stage3.append(third(*pieces[2]))
    query_pass(3)
    stage3 += [third(*piece) for piece in pieces[3:]]

    small_wait(tile_own, tile_all, tile_send, tile_recv)
    tile_all[me] = tile_own[...]
    pack_loss = tile_all[0]
    for j in range(1, members):
        pack_loss = pack_loss + tile_all[j]
    tile_lane = lax.broadcasted_iota(jnp.int32, pack_loss.shape, 1)
    sum_own[...] = jnp.where(tile_lane == 0, pack_loss, length.astype(F32))
    for shift in range(1, groups):
        start(copy(sum_own, sum_all.at[dp], sum_send.at[shift], sum_recv.at[dp], (dp_peer(shift), me)))
    sum_all[dp] = sum_own[...]

    key_pass(0)
    key_pass(1)

    collect = step_a // mine
    is_collector = core == collect
    stage4 = []
    for shift in range(1, members):
        target = patch_peer(shift)
        span = fin_ref.at[:, pl.ds(span_start(target, features), SPAN)]
        stage4.append(copy(span, w4_ref.at[chip], s4.at[shift], r4.at[chip], (dp, target)))

    @pl.when(is_collector)
    def _():
        summed = wz_ref[step_a - core * mine].astype(F32)
        for shift in range(1, outer):
            source = lax.rem(step_a + shift, outer)
            for side, span in enumerate(spans):
                slot = w3_ref.at[source, span]
                copy(slot, slot, s3.at[0, side], r3.at[source, side], (source * 2 + step_b, me)).wait_recv()
            summed = summed + w3_ref[source].astype(F32)
        fin_ref[...] = summed.astype(BF16)
        for item in stage4:
            item.start()
        w4_ref[chip] = fin_ref[:, pl.ds(span_start(me, features), SPAN)]

    key_pass(2)
    key_pass(3)

    for shift in range(1, groups):
        source = dp_peer(shift)
        copy(sum_own, sum_all.at[source], sum_send.at[shift], sum_recv.at[source], (source, me)).wait_recv()
    totals = sum_all[0]
    for j in range(1, groups):
        totals = totals + sum_all[j]
    sum_ref[...] = totals

    def fetched(owner):
        copy(w4_ref.at[owner], w4_ref.at[owner], s4.at[0], r4.at[owner], (dp, partner)).wait_recv()

    @pl.when(jnp.logical_not(is_collector))
    def _():
        fetched(chip)

    for shift in range(1, chips):
        fetched(far(shift))
    shape = (features, SPAN)
    start_lane = me * features - span_start(me, features)
    chosen = (
        lax.broadcasted_iota(jnp.int32, shape, 1) == start_lane + lax.broadcasted_iota(jnp.int32, shape, 0)
    ).astype(F32).astype(BF16)
    result = nt(chosen, w4_ref[0])
    for j in range(1, chips):
        result = result + nt(chosen, w4_ref[j])
    dw_ref[...] = result

    for item in pending:
        item.wait_send()
    for owner, item in stage3:

        @pl.when(owner != step_a)
        def _():
            item.wait_send()

    @pl.when(is_collector)
    def _():
        for item in stage4:
            item.wait_send()


def scale_kernel(slots, total, sum_ref, dq_ref, dk_ref, dv_ref, dw_ref, query_ref, key_ref, value_ref, weight_ref, loss_ref):
    count = sum_ref[0:1, 1:2]
    ratio = slots / count
    query_ref[...] = dq_ref[...] * ratio
    key_ref[...] = dk_ref[...] * ratio
    value_ref[...] = dv_ref[...] * ratio
    weight_ref[...] = dw_ref[...] * (ratio / total)
    loss_ref[...] = sum_ref[0:1, 0:1] / (count * WIDTH)


def solution(mesh):
    members, groups = mesh.shape["patch"], mesh.shape["dp"]

    def local(query_rows, key_rows, value_rows, out_weight, target, lengths, segments):
        rows = query_rows.shape[1]
        total = rows * members
        chips = members // 2
        outer = groups // 2
        mine = outer // 2
        share = WIDTH // groups
        vmem = pl.BlockSpec(memory_space=pltpu.VMEM)
        hbm = pl.BlockSpec(memory_space=pltpu.HBM)
        dma = pltpu.SemaphoreType.DMA
        outs = pl.pallas_call(
            functools.partial(kernel, members, groups),
            out_shape=(
                jax.ShapeDtypeStruct((FEAT, rows), F32),
                jax.ShapeDtypeStruct((FEAT, rows), F32),
                jax.ShapeDtypeStruct((FEAT, rows), F32),
                jax.ShapeDtypeStruct((FEAT // members, share), F32),
                jax.ShapeDtypeStruct((8, 128), F32),
            ),
            in_specs=[pl.BlockSpec(memory_space=pltpu.SMEM)] + [hbm] * 6,
            out_specs=(vmem,) * 5,
            scratch_shapes=[
                pltpu.VMEM((FEAT, WIDTH), BF16),
                pltpu.VMEM((rows, WIDTH), BF16),
                pltpu.VMEM((1, rows), jnp.int32),
                pltpu.VMEM((4, members, FEAT, rows), BF16),
                pltpu.VMEM((8, rows), jnp.int32),
                pltpu.VMEM((members, 8, rows), jnp.int32),
                pltpu.VMEM((2 * HEADS, rows), F32),
                pltpu.VMEM((members, 2 * HEADS, rows), F32),
                pltpu.VMEM((total, 128), F32),
                pltpu.VMEM((total, rows), F32),
                pltpu.VMEM((PAIRS, total, 2 * rows), F32),
                pltpu.VMEM((FEAT_PAD, rows), F32),
                pltpu.VMEM((rows, WIDTH), BF16),
                pltpu.VMEM((groups, share, FEAT_PAD), BF16),
                pltpu.VMEM((groups // 2, share, FEAT_PAD), BF16),
                pltpu.VMEM((mine, share, FEAT_PAD), F32),
                pltpu.VMEM((mine, share, FEAT_PAD), BF16),
                pltpu.VMEM((mine, share, FEAT_PAD), BF16),
                pltpu.VMEM((mine, share, FEAT_PAD), BF16),
                pltpu.VMEM((outer, share, FEAT_PAD), BF16),
                pltpu.VMEM((share, FEAT_PAD), BF16),
                pltpu.VMEM((chips, share, SPAN), BF16),
                pltpu.VMEM((8, 128), F32),
                pltpu.VMEM((members, 8, 128), F32),
                pltpu.VMEM((8, 128), F32),
                pltpu.VMEM((groups, 8, 128), F32),
                dma((6,)),
                dma((4, members, PAIRS)),
                dma((4, members, PAIRS)),
                dma((members,)),
                dma((members,)),
                dma((members,)),
                dma((members,)),
                dma((members,)),
                dma((members,)),
                dma((groups,)),
                dma((groups,)),
                dma,
                dma,
                dma((mine, 2)),
                dma((mine, 2)),
                dma((mine, 2)),
                dma((outer, 2)),
                dma((members,)),
                dma((chips,)),
            ],
            compiler_params=pltpu.CompilerParams(collective_id=0, has_side_effects=True, vmem_limit_bytes=65900000),
            name="sublayer",
        )(
            lengths,
            segments,
            query_rows[0].T,
            key_rows[0].T,
            value_rows[0].T,
            out_weight,
            target[0],
        )
        final = pl.pallas_call(
            functools.partial(scale_kernel, groups * total, total),
            out_shape=(
                jax.ShapeDtypeStruct((FEAT, rows), F32),
                jax.ShapeDtypeStruct((FEAT, rows), F32),
                jax.ShapeDtypeStruct((FEAT, rows), F32),
                jax.ShapeDtypeStruct((FEAT // members, share), F32),
                jax.ShapeDtypeStruct((1, 1), F32),
            ),
            in_specs=[vmem] * 5,
            out_specs=(vmem,) * 5,
            compiler_params=pltpu.CompilerParams(vmem_limit_bytes=65900000),
            name="scale",
        )(outs[4], *outs[:4])
        return (final[0].T[None], final[1].T[None], final[2].T[None], final[3], final[4].reshape(()))

    placed = (
        P("dp", "patch", None),
        P("dp", "patch", None),
        P("dp", "patch", None),
        P(),
        P("dp", "patch", None),
        P("dp"),
        P("dp", "patch"),
    )
    return jax.shard_map(
        local,
        mesh=mesh,
        in_specs=placed,
        out_specs=(
            P("dp", "patch", None),
            P("dp", "patch", None),
            P("dp", "patch", None),
            P("patch", "dp"),
            P(),
        ),
        check_vma=False,
    )
```
